32 devices in a mesh: spin: 2 (over core), band: 8 (over z, x), grid: 2 (over y).
Axes of the slice: x: 2, y: 2, z: 4, core: 2. Of those that a mesh axis runs over, the one named last changes fastest.
Arguments:
- orbitals: bfloat16 [2, 64, 128, 128, 128], P('spin', 'band', 'grid'), may hold values from -0.14941406 to 0.14941406
- partial_bands: int32 [2, 2], P('spin'), may hold values from 0 to 63
- core_density: float32 [128, 128, 128], P('grid'), may hold values from 0.002 to 0.2
Outputs:
- potential: float32 [2, 128, 128, 128], P('spin', 'grid', 'band')
The draws below stay inside these ranges and needn't reach their ends.
Inputs may be any that keep to these rules, and one draw needn't show every extreme that they name: `partial_bands`: row s holds, for spin s, the first half-occupied band and the count of half-occupied bands; bands past 64 - 1 do not exist.
All inputs are finite; a program needn't handle non-finite values.
Results may differ from the reference program's by a relative error of at most 0.0003.
Values sent between devices are 32-bit elements; how exact they have to be, the bound alone decides.
No kernel may reach another device: no remote copies, remote signals or barrier semaphores. Data moves between devices by JAX's collectives and lax.ppermute only.
A program may use at most 128 MiB of HBM per device.

```python
import math
import jax
import jax.numpy as jnp
from jax import lax

NX = 128
NY = 128
NZ = 128
SPINS = 2
BANDS = 64


def set_ends(drawn, own_key, smallest, high):
    extent = drawn.shape
    spot = [jax.random.randint(jax.random.fold_in(own_key, axis), (), 0, extent[axis]) for axis in range(len(extent))]
    drawn = drawn.at[tuple(spot)].set(smallest)
    longest = extent.index(max(extent))
    spot[longest] = (spot[longest] + 1) % extent[longest]
    return drawn.at[tuple(spot)].set(high)


def shard_levels(own_key, shape, pieces, least, top_value):
    def one(axis_at, parts):
        steps = jax.random.uniform(jax.random.fold_in(jax.random.fold_in(own_key, 6), axis_at), (parts,), jnp.float32, least / len(pieces), top_value / len(pieces))
        return jnp.repeat(jnp.exp(steps), shape[axis_at] // parts).reshape((-1,) + (1,) * (len(shape) - axis_at - 1))

    factor_of = one(*pieces[0])
    for cut in pieces[1:]:
        factor_of = factor_of * one(*cut)
    return factor_of


def noise(key, shape, scale, reach, cuts=(), kind=jnp.bfloat16):
    drawn = scale * jax.random.normal(key, shape, jnp.float32)
    if cuts:
        drawn = drawn * shard_levels(key, shape, cuts, -0.22, 0.18)
    return jnp.clip(drawn, -reach, reach).astype(kind)


def setup_inputs(seed: int = 0) -> dict:
    arg_keys = jax.random.split(jax.random.key(seed), 4)
    return {
        "orbitals": noise(arg_keys[0], (SPINS, BANDS, NX, NY, NZ), 0.025, 0.14941406, ((0, 2), (1, 8), (2, 2))),
        "partial_bands": set_ends(jax.random.randint(arg_keys[1], (SPINS, 2), 0, BANDS), jax.random.fold_in(arg_keys[1], 1), 0, BANDS - 1).astype(jnp.int32),
        "core_density": jnp.clip(jnp.exp(math.log(0.2) - 4.6051702 * jax.random.uniform(arg_keys[2], (NX, NY, NZ), jnp.float32) ** shard_levels(arg_keys[2], (NX, NY, NZ), ((0, 2),), -0.2, 0.2)), 0.002, 0.2),
    }


KAPPA = 0.804
MU_X = 0.2195149727645171
BETA = 0.06672455060314922
GAMMA = (1.0 - math.log(2.0)) / math.pi ** 2
FZ_NORM = 2.0 ** (4.0 / 3.0) - 2.0
FPP_ZERO = 1.709921

def pw_fit(radius, amp, alpha, beta_one, beta_two, beta_three, beta_four):
    root = jnp.sqrt(radius)
    denom = 2.0 * amp * (beta_one * root + beta_two * radius + beta_three * radius * root + beta_four * radius * radius)
    return -2.0 * amp * (1.0 + alpha * radius) * jnp.log(1.0 + 1.0 / denom)

def exchange_part(double, sigma_four):
    kfermi = (3.0 * math.pi ** 2 * double) ** (1.0 / 3.0)
    scaled = sigma_four / (4.0 * kfermi * kfermi * double * double)
    enhance = 1.0 + KAPPA - KAPPA / (1.0 + MU_X * scaled / KAPPA)
    return -0.75 / math.pi * kfermi * double * enhance

def xc_energy(n_up, n_down, s_uu, s_ud, s_dd):
    exch = 0.5 * (exchange_part(2.0 * n_up, 4.0 * s_uu) + exchange_part(2.0 * n_down, 4.0 * s_dd))
    total = n_up + n_down
    zeta = (n_up - n_down) / total
    radius = (3.0 / (4.0 * math.pi * total)) ** (1.0 / 3.0)
    ec_para = pw_fit(radius, 0.031091, 0.2137, 7.5957, 3.5876, 1.6382, 0.49294)
    ec_ferro = pw_fit(radius, 0.015545, 0.20548, 14.1189, 6.1977, 3.3662, 0.62517)
    neg_stiff = pw_fit(radius, 0.016887, 0.11125, 10.357, 3.6231, 0.88026, 0.49671)
    plus_z = 1.0 + zeta
    minus_z = 1.0 - zeta
    fzeta = (plus_z ** (4.0 / 3.0) + minus_z ** (4.0 / 3.0) - 2.0) / FZ_NORM
    zeta_four = zeta ** 4
    ec_lda = ec_para - neg_stiff * fzeta / FPP_ZERO * (1.0 - zeta_four) + (ec_ferro - ec_para) * fzeta * zeta_four
    phi = 0.5 * (plus_z ** (2.0 / 3.0) + minus_z ** (2.0 / 3.0))
    phi_cube = phi * phi * phi
    kfermi = (3.0 * math.pi ** 2 * total) ** (1.0 / 3.0)
    screen_sq = 4.0 * kfermi / math.pi
    sigma = s_uu + 2.0 * s_ud + s_dd
    tsq = sigma / (4.0 * phi * phi * screen_sq * total * total)
    amp = BETA / GAMMA / (jnp.exp(-ec_lda / (GAMMA * phi_cube)) - 1.0)
    atsq = amp * tsq
    gradient_term = GAMMA * phi_cube * jnp.log(1.0 + BETA / GAMMA * tsq * (1.0 + atsq) / (1.0 + atsq + atsq * atsq))
    return exch + total * (ec_lda + gradient_term)

def spectral(field, axis):
    length = field.shape[axis]
    index = jnp.arange(length, dtype=jnp.int32)
    mode = jnp.where(index < length // 2, index, index - length)
    mode = jnp.where(index == length // 2, 0, mode)
    wave = 2.0 * math.pi / length * mode.astype(jnp.float32)
    shape = [1, 1, 1]
    shape[axis] = length
    spec = jnp.fft.fft(field, axis=axis)
    return jnp.real(jnp.fft.ifft(spec * (1j * wave.reshape(shape)), axis=axis)).astype(jnp.float32)

def reference(orbitals, partial_bands, core_density):
    band_ids = jnp.arange(BANDS, dtype=jnp.int32)

    def spin_density(spin_id):
        first = partial_bands[spin_id, 0]
        span = partial_bands[spin_id, 1]
        weights = jnp.where((band_ids >= first) & (band_ids < first + span), 0.5, 1.0).astype(jnp.float32)

        def accumulate(total, item):
            weight, orbital = item
            values = orbital.astype(jnp.float32)
            return (total + weight * values * values, None)
        start = jnp.zeros((NX, NY, NZ), jnp.float32)
        total, unused = lax.scan(accumulate, start, (weights, orbitals[spin_id]))
        return total + 0.5 * core_density
    dens_up = spin_density(0)
    dens_down = spin_density(1)
    grad_up = [spectral(dens_up, axis) for axis in range(3)]
    grad_down = [spectral(dens_down, axis) for axis in range(3)]
    s_uu = grad_up[0] * grad_up[0] + grad_up[1] * grad_up[1] + grad_up[2] * grad_up[2]
    s_ud = grad_up[0] * grad_down[0] + grad_up[1] * grad_down[1] + grad_up[2] * grad_down[2]
    s_dd = grad_down[0] * grad_down[0] + grad_down[1] * grad_down[1] + grad_down[2] * grad_down[2]
    energy, pull = jax.vjp(xc_energy, dens_up, dens_down, s_uu, s_ud, s_dd)
    derivs = pull(jnp.ones_like(energy))
    div_up = jnp.zeros_like(dens_up)
    div_down = jnp.zeros_like(dens_up)
    for axis in range(3):
        flux_up = 2.0 * derivs[2] * grad_up[axis] + derivs[3] * grad_down[axis]
        flux_down = 2.0 * derivs[4] * grad_down[axis] + derivs[3] * grad_up[axis]
        div_up = div_up + spectral(flux_up, axis)
        div_down = div_down + spectral(flux_down, axis)
    return jnp.stack([derivs[0] - div_up, derivs[1] - div_down])
```

```python
import math

import jax
import jax.numpy as jnp
import numpy as np
from jax import lax
from jax.sharding import PartitionSpec as P

KAPPA = 0.804
MU_X = 0.2195149727645171
BETA = 0.06672455060314922
GAMMA = (1.0 - math.log(2.0)) / math.pi**2
FZ_NORM = 2.0 ** (4.0 / 3.0) - 2.0
FPP_ZERO = 1.709921
NEAR = lax.Precision.HIGH


def pw_fit(radius, amp, alpha, beta_one, beta_two, beta_three, beta_four):
    root = jnp.sqrt(radius)
    denom = (
        2.0
        * amp
        * (
            beta_one * root
            + beta_two * radius
            + beta_three * radius * root
            + beta_four * radius * radius
        )
    )
    return -2.0 * amp * (1.0 + alpha * radius) * jnp.log(1.0 + 1.0 / denom)


def exchange_part(double, sigma_four):
    kfermi = (3.0 * math.pi**2 * double) ** (1.0 / 3.0)
    scaled = sigma_four / (4.0 * kfermi * kfermi * double * double)
    enhance = 1.0 + KAPPA - KAPPA / (1.0 + MU_X * scaled / KAPPA)
    return -0.75 / math.pi * kfermi * double * enhance


def xc_energy(n_up, n_down, s_uu, s_ud, s_dd):
    exch = 0.5 * (exchange_part(2.0 * n_up, 4.0 * s_uu) + exchange_part(2.0 * n_down, 4.0 * s_dd))
    total = n_up + n_down
    zeta = (n_up - n_down) / total
    radius = (3.0 / (4.0 * math.pi * total)) ** (1.0 / 3.0)
    ec_para = pw_fit(radius, 0.031091, 0.2137, 7.5957, 3.5876, 1.6382, 0.49294)
    ec_ferro = pw_fit(radius, 0.015545, 0.20548, 14.1189, 6.1977, 3.3662, 0.62517)
    neg_stiff = pw_fit(radius, 0.016887, 0.11125, 10.357, 3.6231, 0.88026, 0.49671)
    plus_z = 1.0 + zeta
    minus_z = 1.0 - zeta
    fzeta = (plus_z ** (4.0 / 3.0) + minus_z ** (4.0 / 3.0) - 2.0) / FZ_NORM
    zeta_four = zeta**4
    ec_lda = (
        ec_para
        - neg_stiff * fzeta / FPP_ZERO * (1.0 - zeta_four)
        + (ec_ferro - ec_para) * fzeta * zeta_four
    )
    phi = 0.5 * (plus_z ** (2.0 / 3.0) + minus_z ** (2.0 / 3.0))
    phi_cube = phi * phi * phi
    kfermi = (3.0 * math.pi**2 * total) ** (1.0 / 3.0)
    screen_sq = 4.0 * kfermi / math.pi
    sigma = s_uu + 2.0 * s_ud + s_dd
    tsq = sigma / (4.0 * phi * phi * screen_sq * total * total)
    amp = BETA / GAMMA / (jnp.exp(-ec_lda / (GAMMA * phi_cube)) - 1.0)
    atsq = amp * tsq
    gradient_term = (
        GAMMA
        * phi_cube
        * jnp.log(1.0 + BETA / GAMMA * tsq * (1.0 + atsq) / (1.0 + atsq + atsq * atsq))
    )
    return exch + total * (ec_lda + gradient_term)


def deriv_table(length):
    index = np.arange(length)
    mode = np.where(index < length // 2, index, index - length)
    mode = np.where(2 * index == length, 0, mode)
    wave = 2.0 * np.pi / length * mode
    angle = 2.0 * np.pi / length * (index[:, None] * index[None, :] % length)
    sines, cosines = np.sin(angle), np.cos(angle)
    return ((cosines * wave) @ sines.T - (sines * wave) @ cosines.T) / length


def xor_swap(block, axis, mask):
    count = lax.axis_size(axis)
    return lax.ppermute(block, axis, [(low, low ^ mask) for low in range(count)])


def pick(block, dim, at):
    return lax.dynamic_index_in_dim(block, at, dim, keepdims=False)


def halved(block, dim, bit, position):
    sent = pick(block, dim, 1 - bit)
    return pick(block, dim, bit) + xor_swap(sent, "band", 1 << position)


def per_device(orbitals, partial_bands, core_density):
    states = orbitals[0]
    count_local, x_rows, y_cols, z_cells = states.shape
    bands, grids = lax.axis_size("band"), lax.axis_size("grid")
    band_at, grid_at = lax.axis_index("band"), lax.axis_index("grid")
    lines = bands // 2
    levels = lines.bit_length() - 1
    side, line = band_at % 2, band_at // 2
    y_block = y_cols // bands
    rows = x_rows // lines
    chunks = min(4, rows)
    deep = rows // chunks

    table_x = deriv_table(x_rows * grids)
    table_y = deriv_table(y_cols)
    table_z = jnp.asarray(deriv_table(z_cells), jnp.float32)

    band_ids = band_at * count_local + jnp.arange(count_local, dtype=jnp.int32)
    first_band, span = partial_bands[0, 0], partial_bands[0, 1]
    weights = jnp.where((band_ids >= first_band) & (band_ids < first_band + span), 0.5, 1.0).astype(
        jnp.float32
    )
    view = states.reshape(count_local, lines, chunks, deep, lines, 2, y_block, z_cells)
    line_bits = [(line >> level) & 1 for level in range(levels)]

    def scatter(chunk):
        values = view[:, :, chunk].astype(jnp.float32)
        part = jnp.sum(weights.reshape((-1,) + (1,) * 6) * values * values, axis=0)
        part = lax.optimization_barrier(part)
        part = part.reshape((2,) * levels + part.shape[1:])
        left = list(range(levels))
        if chunk == 0 and levels > 0:
            part = halved(part, levels - 1, line_bits[0], 1)
            left = left[1:]
        part = halved(part, part.ndim - 3, side, 0)
        for level in left:
            at = levels - 1 - level
            part = halved(part, at, line_bits[level], 1 + level)
        return part

    mine = jnp.stack([scatter(chunk) for chunk in range(chunks)], axis=0)
    core_part = core_density.reshape(lines, rows, lines, 2, y_block, z_cells)
    core_part = pick(pick(core_part, 4 - 1, side), 0, line)
    mine = mine.reshape(rows, lines, y_block, z_cells) + 0.5 * core_part

    beside = xor_swap(mine, "band", 1)
    own_first = np.stack(
        [
            np.concatenate(
                [
                    table_y.reshape(lines, 2, y_block, lines, 2, y_block)[:, par, :, :, par],
                    table_y.reshape(lines, 2, y_block, lines, 2, y_block)[:, par, :, :, 1 - par],
                ],
                axis=2,
            ).reshape(y_cols // 2, y_cols)
            for par in range(2)
        ]
    )
    table_h = pick(jnp.asarray(own_first, jnp.float32), 0, side)
    half_lines = lambda block: block.reshape(rows, y_cols // 2, z_cells)
    steep_y = jnp.einsum(
        "jl,rlz->rjz",
        table_h,
        jnp.concatenate([half_lines(mine), half_lines(beside)], axis=1),
        precision=NEAR,
    ).reshape(mine.shape)

    def to_blocks(block):
        pieces = [pick(block, 1, line)]
        for mask in range(1, lines):
            pieces.append(xor_swap(pick(block, 1, line ^ mask), "band", 2 * mask))
        return pieces

    own = jnp.concatenate(to_blocks(mine), axis=0)
    steep_y = jnp.concatenate(to_blocks(steep_y), axis=0)

    tx = table_x.reshape(grids, lines, rows, grids, lines, rows)
    order = [[at ^ k for k in range(lines)] for at in range(lines)]
    gorder = [[at ^ k for k in range(grids)] for at in range(grids)]
    tables_x = np.stack(
        [
            tx[g][order[s]][:, :, gorder[g]][:, :, :, order[s]].reshape(x_rows, x_rows * grids)
            for g in range(grids)
            for s in range(lines)
        ]
    )
    table_xl = pick(jnp.asarray(tables_x, jnp.float32), 0, grid_at * lines + line)

    def along_x(block):
        every = [block] + [xor_swap(block, "grid", mask) for mask in range(1, grids)]
        return jnp.einsum(
            "jl,lyz->jyz", table_xl, jnp.concatenate(every, axis=0), precision=NEAR
        )

    def along_z(block):
        return jnp.einsum("xyl,jl->xyj", block, table_z, precision=NEAR)

    steep = [along_x(own), steep_y, along_z(own)]
    other = xor_swap(own, "spin", 1)
    other_steep = [xor_swap(item, "spin", 1) for item in steep]
    is_up = lax.axis_index("spin") == 0
    dens_up = jnp.where(is_up, own, other)
    dens_down = jnp.where(is_up, other, own)
    s_own = sum(a * a for a in steep)
    s_other = sum(a * a for a in other_steep)
    s_ud = sum(a * b for a, b in zip(steep, other_steep))
    s_uu = jnp.where(is_up, s_own, s_other)
    s_dd = jnp.where(is_up, s_other, s_own)
    energy, pull = jax.vjp(xc_energy, dens_up, dens_down, s_uu, s_ud, s_dd)
    derivs = pull(jnp.ones_like(energy))
    dn_own = jnp.where(is_up, derivs[0], derivs[1])
    ds_own = jnp.where(is_up, derivs[2], derivs[4])
    flux = [2.0 * ds_own * a + derivs[3] * b for a, b in zip(steep, other_steep)]
    flux, dn_own = lax.optimization_barrier((flux, dn_own))
    div_z = lax.optimization_barrier(along_z(flux[2]))

    half = x_rows // bands
    ty = table_y.reshape(bands, y_block, bands, y_block)
    border = [[at ^ k for k in range(bands)] for at in range(bands)]
    tables_y = np.stack(
        [ty[border[b]][:, :, border[b]].reshape(y_cols, y_cols) for b in range(bands)]
    )
    table_yl = pick(jnp.asarray(tables_y, jnp.float32), 0, band_at)
    out_y = flux[1].reshape(lines, 2, half, y_block, z_cells)
    pieces = []
    for mask in range(bands):
        piece = pick(out_y[mask // 2], 0, side ^ (mask % 2))
        pieces.append(xor_swap(piece, "band", mask) if mask else piece)
    whole_lines = jnp.stack(pieces, axis=1).reshape(half, y_cols, z_cells)
    div_y = jnp.einsum("jl,rlz->rjz", table_yl, whole_lines, precision=NEAR)
    div_y = div_y.reshape(half, bands, y_block, z_cells)
    back = [xor_swap(div_y[:, mask], "band", mask) if mask else div_y[:, 0] for mask in range(bands)]
    div_y = jnp.stack(
        [
            jnp.stack([pick(jnp.stack(back[2 * k : 2 * k + 2]), 0, side ^ par) for par in range(2)])
            for k in range(lines)
        ]
    ).reshape(own.shape)

    div_x = lax.optimization_barrier(along_x(flux[0]))
    potential = dn_own - (div_x + div_y + div_z)
    potential = potential.reshape(lines, rows, y_block, z_cells)
    ordered = jnp.stack([pick(potential, 0, line ^ at) for at in range(lines)])
    return ordered.reshape(1, x_rows, y_block, z_cells)


def solution(mesh):
    in_specs = (P("spin", "band", "grid", None, None), P("spin", None), P("grid", None, None))
    out_specs = P("spin", "grid", "band", None)
    return jax.shard_map(
        per_device, mesh=mesh, in_specs=in_specs, out_specs=out_specs, check_vma=False
    )
```
